128 devices in a mesh: vocab: 128 (over y, z, x, core).
Axes of the slice: x: 4, y: 4, z: 4, core: 2. Of those that a mesh axis runs over, the one named last changes fastest.
Arguments:
- draft_ids: int32 [128, 8], P('vocab'), may hold values from 0 to 262143, as said below
- draft_len: int32 [128], P('vocab'), may hold values from 1 to 8
- accepted: int32 [128], P('vocab'), may hold values from 1 to 8
- targets: int32 [128, 8], P('vocab'), may hold values from 0 to 262143
- hidden: bfloat16 [128, 8, 2048], P('vocab'), may hold values from -6 to 6
- ple_table: bfloat16 [262144, 512], P('vocab'), may hold values from -6 to 6
- gate_proj: bfloat16 [2, 2048, 256], replicated, may hold values from -0.125 to 0.125
- out_proj: bfloat16 [2, 256, 2048], replicated, may hold values from -0.375 to 0.375
- post_gain: float32 [2, 2048], replicated, may hold values from 0.25 to 1.75
- final_gain: float32 [2048], replicated, may hold values from 0.25 to 1.75
- embedding: bfloat16 [262144, 2048], P('vocab'), may hold values from -0.44921875 to 0.44921875
Outputs:
- token_logprob: float32 [128, 8], P('vocab')
- seq_logprob: float32 [128], P('vocab')
The draws below stay inside these ranges and needn't reach their ends.
Inputs may be any that keep to these rules, and one draw needn't show every extreme that they name: `draft_ids`: among the 8 draft ids of one device's sequences, at most 2 lie in any one aligned block of 2048 vocabulary entries, and in every draw some block holds exactly 2 of them.
All inputs are finite; a program needn't handle non-finite values.
Results may differ from the reference program's by a relative error of at most 0.00096.
Values may be sent and summed in bfloat16 or wider, within the bound.
A program may use at most 64 MiB of HBM per device.

```python
import math
import jax
import jax.numpy as jnp
import numpy as np
from jax import lax

D = 2048
PLE_DIM = 256
VOC_DEV = 2048
LAYERS = 2
DRAFT = 8
MOST = 2
SEQ_DEV = 1
VOCAB = 262144
SEQS = 128
PLE_W = 512
N_VOCAB = 128


def device_block(key):
    count = SEQ_DEV * DRAFT
    first, second, third, fourth = jax.random.split(key, 4)
    holders = jax.random.permutation(first, N_VOCAB).astype(jnp.int32)
    slots = jnp.arange(count, dtype=jnp.int32) // MOST
    holder_of = holders[slots]
    shuffle = jax.random.permutation(second, count)
    holder_of = holder_of[shuffle]
    lower = jax.random.randint(third, (count,), 0, VOC_DEV, dtype=jnp.int32)
    upper = jax.random.randint(fourth, (count,), 0, VOC_DEV, dtype=jnp.int32)
    within = jnp.minimum(lower, upper)
    return holder_of * VOC_DEV + within


def draw_draft_ids(key, part):
    keys = jax.random.split(jax.random.fold_in(key, 17), N_VOCAB)
    blocks = jax.vmap(device_block)(keys)
    return blocks.reshape(SEQS, DRAFT)


def set_ends(drawn, stream_key, low, high):
    dims = drawn.shape
    index_at = [jax.random.randint(jax.random.fold_in(stream_key, axis), (), 0, dims[axis]) for axis in range(len(dims))]
    drawn = drawn.at[tuple(index_at)].set(low)
    longest = dims.index(max(dims))
    index_at[longest] = (index_at[longest] + 1) % dims[longest]
    return drawn.at[tuple(index_at)].set(high)


def block_levels(rng, dims, cuts, least, largest):
    factor_of, own = 1.0, jax.random.fold_in(rng, 6)
    for axis_at, shards_of in cuts:
        draws = jnp.exp(jax.random.uniform(jax.random.fold_in(own, axis_at), (shards_of,), jnp.float32, least / len(cuts), largest / len(cuts)))
        factor_of = factor_of * jnp.repeat(draws, dims[axis_at] // shards_of).reshape([-1 if axis == axis_at else 1 for axis in range(len(dims))])
    return factor_of


def ranked_wide(stream_key, extent, count, lean):
    portions = [min(1 << octave, count + 1 - (1 << octave)) * (1 << 20) // math.isqrt((1 << octave) ** lean) + 1 for octave in range((count + 1).bit_length()) if 1 << octave <= count]
    spread = 1 + sum(portions) // (1 << 30)
    table = np.cumsum(np.array([max(1, weight // spread) for weight in portions]))
    ticket = jax.random.randint(jax.random.fold_in(stream_key, 1), extent, 0, int(table[len(portions) - 1]))
    start = jnp.left_shift(1, jnp.searchsorted(jnp.asarray(table, jnp.int32), ticket, side="right").astype(jnp.int32))
    grade = start - 1 + jax.random.randint(jax.random.fold_in(stream_key, 4), extent, 0, 1 << 30) % jnp.minimum(start, count + 1 - start)
    return jax.random.permutation(jax.random.fold_in(stream_key, 2), count)[grade].astype(jnp.int32)


def scatter_about(own_key, shape, scale, most, cuts=(), held_as=jnp.bfloat16):
    array = jax.random.normal(own_key, shape, jnp.float32) * scale
    if len(cuts) > 0:
        array = block_levels(own_key, shape, cuts, -0.22, 0.18) * array
    return jnp.clip(array, min=-most, max=most).astype(held_as)


def setup_inputs(seed: int = 0) -> dict:
    key_list = jax.random.split(jax.random.key(seed), 12)
    return {
        "draft_ids": draw_draft_ids(jax.random.fold_in(key_list[11], 71), 0),
        "draft_len": set_ends(jax.random.randint(key_list[1], (SEQS,), 1, DRAFT + 1), jax.random.fold_in(key_list[1], 1), 1, DRAFT).astype(jnp.int32),
        "accepted": set_ends(jax.random.randint(key_list[2], (SEQS,), 1, DRAFT + 1), jax.random.fold_in(key_list[2], 1), 1, DRAFT).astype(jnp.int32),
        "targets": set_ends(ranked_wide(key_list[3], (SEQS, DRAFT), VOCAB, 1), jax.random.fold_in(key_list[3], 3), 0, VOCAB - 1).astype(jnp.int32),
        "hidden": scatter_about(key_list[4], (SEQS, DRAFT, D), 1.0, 6.0, ((0, 128),)),
        "ple_table": scatter_about(key_list[5], (VOCAB, PLE_W), 1.0, 6.0, ((0, 128),)),
        "gate_proj": scatter_about(key_list[6], (LAYERS, D, PLE_DIM), D ** -0.5, 0.125),
        "out_proj": scatter_about(key_list[7], (LAYERS, PLE_DIM, D), PLE_DIM ** -0.5, 0.375),
        "post_gain": jnp.clip(1.0 + 0.15 * jax.random.normal(key_list[8], (LAYERS, D), jnp.float32), 0.25, 1.75),
        "final_gain": jnp.clip(1.0 + 0.15 * jax.random.normal(key_list[9], (D,), jnp.float32), 0.25, 1.75),
        "embedding": scatter_about(key_list[10], (VOCAB, D), 0.07, 0.44921875, ((0, 128),)),
    }


def rms_norm(value):
    return value / jnp.sqrt(lax.optimization_barrier(jnp.mean(value * value, axis=-1, keepdims=True)) + 1e-06)

def reference(draft_ids, draft_len, accepted, targets, hidden, ple_table, gate_proj, out_proj, post_gain, final_gain, embedding):
    seqs, draft = draft_ids.shape
    width = hidden.shape[2]
    place = lax.iota(jnp.int32, draft)[None, :]
    live = (place < draft_len[:, None]).reshape(seqs * draft, 1)
    rows = jnp.take(ple_table, draft_ids.reshape(-1), axis=0)
    ple = jnp.where(live, rows, jnp.zeros_like(rows)).astype(jnp.bfloat16)
    state = hidden.reshape(seqs * draft, width)
    inner = gate_proj.shape[2]
    for layer in range(gate_proj.shape[0]):
        gated = jax.nn.gelu(jnp.dot(state, gate_proj[layer], preferred_element_type=jnp.float32), approximate=True)
        gated = (gated * ple[:, layer * inner:(layer + 1) * inner].astype(jnp.float32)).astype(jnp.bfloat16)
        branch = jnp.dot(gated, out_proj[layer], preferred_element_type=jnp.float32)
        state = (state.astype(jnp.float32) + post_gain[layer] * rms_norm(branch)).astype(jnp.bfloat16)
    normed = (final_gain * rms_norm(state.astype(jnp.float32))).astype(jnp.bfloat16)
    flat_targets = targets.reshape(-1)
    voc_block = embedding.shape[0] // N_VOCAB
    tables = embedding.reshape(N_VOCAB, voc_block, width)

    def step(carry, inputs):
        block, index = inputs
        total, picked = carry
        logits = lax.dot_general(normed, block, (((1,), (1,)), ((), ())), preferred_element_type=jnp.float32)
        logits = 30.0 * jnp.tanh(logits / 30.0)
        total = total + lax.optimization_barrier(jnp.sum(jnp.exp(logits), axis=1))
        columns = index * voc_block + lax.iota(jnp.int32, voc_block)
        picked = picked + lax.optimization_barrier(jnp.sum(jnp.where(columns[None, :] == flat_targets[:, None], logits, 0.0), axis=1))
        return ((total, picked), None)
    count = seqs * draft
    start = (jnp.zeros((count,), jnp.float32), jnp.zeros((count,), jnp.float32))
    (total, picked), _ = lax.scan(step, start, (tables, lax.iota(jnp.int32, N_VOCAB)))
    logprob = (picked - jnp.log(total)).reshape(seqs, draft)
    keep = place < jnp.minimum(accepted, draft_len)[:, None]
    token_logprob = jnp.where(keep, logprob, 0.0)
    return (token_logprob, lax.optimization_barrier(jnp.sum(token_logprob, axis=1)))
```

```python
import jax
import jax.numpy as jnp
from jax import lax
from jax.experimental import pallas as pl
from jax.experimental.pallas import tpu as pltpu
from jax.sharding import PartitionSpec as P

MESH = pl.DeviceIdType.MESH
CHIPS = 64
DRAFT = 8
VOC = 2048
D = 2048
PLE = 256
BLOCK = 256
PARTS = ((0, 768), (768, 640), (1408, 640))
ORDERS = ((0, 1, 2), (1, 2, 0), (2, 0, 1))


def kernel(
    ids_s,
    targets_s,
    len_s,
    acc_s,
    hidden_ref,
    post_ref,
    final_ref,
    table_hbm,
    gate_hbm,
    outp_hbm,
    emb_hbm,
    tok_ref,
    seq_ref,
    emb_v,
    table_v,
    gate_v,
    outp_v,
    msg,
    inbox,
    lookup,
    packed,
    arrived,
    gath,
    states,
    even,
    odd,
    res_out,
    res_in,
    load_sem,
    pair_send,
    pair_recv,
    id_sem,
    row_sem,
    res_sem,
    send_sem,
    recv_sem,
):
    me = lax.axis_index("vocab")
    core = me % 2
    chip = me // 2
    sibling = me + 1 - 2 * core
    where_am_i = (chip // 16, (chip // 4) % 4, chip % 4)

    def plane(step):
        return ((chip + step) % CHIPS) * 2 + core

    barrier = pltpu.get_barrier_semaphore()

    def greet(step, carry):
        pl.semaphore_signal(barrier, inc=1, device_id=(plane(step),), device_id_type=MESH)
        return carry

    lax.fori_loop(1, CHIPS, greet, 0)
    pl.semaphore_signal(barrier, inc=1, device_id=(sibling,), device_id_type=MESH)

    loads = [
        pltpu.make_async_copy(gate_hbm, gate_v, load_sem.at[0]),
        pltpu.make_async_copy(outp_hbm, outp_v, load_sem.at[1]),
        pltpu.make_async_copy(table_hbm, table_v.at[core], load_sem.at[2]),
        pltpu.make_async_copy(emb_hbm, emb_v.at[core], load_sem.at[3]),
    ]
    for load in loads:
        load.start()

    ids = [ids_s[0, j] for j in range(DRAFT)]
    lane = lax.broadcasted_iota(jnp.int32, (1, 128), 1)
    id_row = jnp.zeros((1, 128), jnp.int32)
    target_row = jnp.zeros((1, 128), jnp.int32)
    for j in range(DRAFT):
        id_row = jnp.where(lane == j, ids[j], id_row)
        target_row = jnp.where(lane % DRAFT == j, targets_s[0, j], target_row)
    msg[0:1, 0:128] = id_row
    msg[0:1, 128:256] = target_row
    inbox[chip, 0:1, 0:128] = id_row
    inbox[chip, 0:1, 128:256] = target_row

    state = hidden_ref[0]
    loads[0].wait()
    first_gate = jnp.dot(state, gate_v[0], preferred_element_type=jnp.float32)

    pl.semaphore_wait(barrier, CHIPS)

    def send_ids(step, carry):
        pltpu.make_async_remote_copy(
            src_ref=msg,
            dst_ref=inbox.at[chip],
            send_sem=id_sem.at[0],
            recv_sem=id_sem.at[1],
            device_id=(plane(step),),
            device_id_type=MESH,
        ).start()
        return carry

    lax.fori_loop(1, CHIPS, send_ids, 0)
    pair = [
        pltpu.make_async_remote_copy(
            src_ref=source,
            dst_ref=target.at[core],
            send_sem=pair_send.at[k],
            recv_sem=pair_recv.at[k],
            device_id=(sibling,),
            device_id_type=MESH,
        )
        for k, (source, target) in enumerate(((table_hbm, table_v), (emb_hbm, emb_v)))
    ]
    for copy in pair:
        copy.start()

    most = pl.ds(0, CHIPS - 1)

    def wait_all(ref, sem):
        pltpu.make_async_copy(ref.at[most], ref.at[most], sem).wait()

    wait_all(inbox, id_sem.at[1])
    everyone = inbox[:, 0, :]

    all_ids = everyone[:, 0:128]
    lanes = lax.broadcasted_iota(jnp.int32, (CHIPS, 128), 1)
    far = DRAFT * VOC
    voc_lane = lax.broadcasted_iota(jnp.int32, (2 * CHIPS, VOC), 1)
    loads[2].wait()
    pair[0].wait_recv()
    for block in range(2):
        local = all_ids - (chip * 2 + block) * VOC
        hit = (lanes < DRAFT) & (local >= 0) & (local < VOC)
        key = lanes * VOC + local
        first = jnp.min(jnp.where(hit, key, far).astype(jnp.float32), axis=1, keepdims=True)
        last = jnp.max(jnp.where(hit, key, -1).astype(jnp.float32), axis=1, keepdims=True)
        one = jnp.where(first < far, first.astype(jnp.int32) & (VOC - 1), -1)
        two = jnp.where(last > first, last.astype(jnp.int32) & (VOC - 1), -1)
        wanted = jnp.concatenate([one, two], axis=0)
        onehot = jnp.where(voc_lane == wanted, 1.0, 0.0).astype(jnp.bfloat16)
        rows = jnp.dot(onehot, table_v[block], preferred_element_type=jnp.float32)
        for slot in range(2):
            for quarter in range(4):
                lookup[pl.ds((block * 2 + slot) * 4 + quarter, CHIPS, stride=16), :] = rows[
                    slot * CHIPS : (slot + 1) * CHIPS, quarter * 128 : (quarter + 1) * 128
                ]
    packed[...] = lookup[...].astype(jnp.bfloat16).reshape(CHIPS, 16, 128)

    def send_rows(step, carry):
        to = (chip + step) % CHIPS
        pltpu.make_async_remote_copy(
            src_ref=packed.at[to],
            dst_ref=arrived.at[chip],
            send_sem=row_sem.at[0],
            recv_sem=row_sem.at[1],
            device_id=(to * 2 + core,),
            device_id_type=MESH,
        ).start()
        return carry

    lax.fori_loop(1, CHIPS, send_rows, 0)
    arrived[chip] = packed[chip]

    sub = lax.broadcasted_iota(jnp.int32, (32, 1), 0)
    holders = [ids[j] // VOC for j in range(DRAFT)]
    place = jnp.zeros((32, 1), jnp.int32)
    for j in range(DRAFT):
        again = jnp.int32(0)
        for i in range(j):
            again = again | (holders[i] == holders[j]).astype(jnp.int32)
        start = holders[j] * 8 + again * 4
        place = jnp.where(sub % DRAFT == j, start, place)
    place = jnp.where(sub % DRAFT < len_s[0], place + sub // DRAFT, -1)
    slots = lax.broadcasted_iota(jnp.int32, (32, CHIPS * 16), 1)
    picker = jnp.where(slots == place, 1.0, 0.0).astype(jnp.bfloat16)
    wait_all(arrived, row_sem.at[1])
    quarters = jnp.dot(
        picker, arrived[...].reshape(CHIPS * 16, 128), preferred_element_type=jnp.float32
    )
    ple = jnp.concatenate([quarters[8 * q : 8 * q + 8] for q in range(4)], axis=1)

    loads[1].wait()
    for layer in range(2):
        if layer == 0:
            gate = first_gate
        else:
            gate = jnp.dot(state, gate_v[layer], preferred_element_type=jnp.float32)
        gated = jax.nn.gelu(gate, approximate=True)
        gated = (gated * ple[:, layer * PLE : (layer + 1) * PLE]).astype(jnp.bfloat16)
        branch = jnp.dot(gated, outp_v[layer], preferred_element_type=jnp.float32)
        scale = lax.rsqrt(jnp.mean(branch * branch, axis=-1, keepdims=True) + 1e-06)
        state = (
            state.astype(jnp.float32) + post_ref[layer : layer + 1, :] * (branch * scale)
        ).astype(jnp.bfloat16)
    wide = state.astype(jnp.float32)
    scale = lax.rsqrt(jnp.mean(wide * wide, axis=-1, keepdims=True) + 1e-06)
    normed = (final_ref[...].reshape(1, D) * (wide * scale)).astype(jnp.bfloat16)
    gath[where_am_i[0], where_am_i[1], where_am_i[2]] = normed

    sent = []

    def view(part, index):
        start, size = PARTS[part]
        return gath.at[index[0], index[1], index[2], :, pl.ds(start, size)]

    def towards(axis, step):
        place = list(where_am_i)
        place[axis] = (place[axis] + step) % 4
        return (((place[0] * 4 + place[1]) * 4 + place[2]) * 2 + core,)

    def send(part, index, axis, step, slot):
        copy = pltpu.make_async_remote_copy(
            src_ref=view(part, index),
            dst_ref=view(part, index),
            send_sem=send_sem.at[len(sent)],
            recv_sem=recv_sem.at[part, slot],
            device_id=towards(axis, step),
            device_id_type=MESH,
        )
        copy.start()
        sent.append(copy)

    def arrival(part, index, slot):
        ref = view(part, index)
        pltpu.make_async_copy(ref, ref, recv_sem.at[part, slot]).wait()

    def slab(part, level, half=None, shift=0):
        order = ORDERS[part]
        index = list(where_am_i)
        for k in range(level):
            index[order[k]] = pl.ds(0, 4)
        if half is not None:
            index[order[0]] = pl.ds(2 * half, 2)
        index[order[level]] = (index[order[level]] + shift) % 4
        return tuple(index)

    for part in range(3):
        for k, step in enumerate((2, 1, 3)):
            send(part, where_am_i, ORDERS[part][0], step, k)
    for level in (1, 2):
        base = 3 + 4 * (level - 1)
        for part in range(3):
            axis = ORDERS[part][level]
            if level == 1:
                for k in range(3):
                    arrival(part, where_am_i, k)
            else:
                arrival(part, slab(part, 1, 0), base - 2)
                arrival(part, slab(part, 1, 1), base - 1)
            send(part, slab(part, level), axis, 1, base)
            send(part, slab(part, level), axis, 3, base + 1)
        for part in range(3):
            axis = ORDERS[part][level]
            arrival(part, slab(part, level, None, 3), base)
            send(part, slab(part, level, 0, 3), axis, 1, base + 2)
            arrival(part, slab(part, level, None, 1), base + 1)
            send(part, slab(part, level, 1, 1), axis, 3, base + 3)
    for part in range(3):
        arrival(part, slab(part, 2, 0), 9)
        arrival(part, slab(part, 2, 1), 10)

    states[...] = gath[...].reshape(CHIPS * DRAFT, D)
    own_lane = lane // DRAFT
    sub16 = lax.broadcasted_iota(jnp.int32, (16, 128), 0)
    targets = jnp.concatenate(
        [
            jnp.sum(
                jnp.where(
                    sub16 == own_lane, everyone[16 * k : 16 * k + 16, 128:256], 0
                ).astype(jnp.float32),
                axis=0,
                keepdims=True,
            )
            for k in range(4)
        ],
        axis=1,
    ).astype(jnp.int32) - chip * (2 * VOC)
    row = lax.broadcasted_iota(jnp.int32, (BLOCK, CHIPS * DRAFT), 0)

    def fold(value):
        return jnp.sum(value.reshape(BLOCK // 8, 8, CHIPS * DRAFT), axis=0)

    def product(index, out):
        block = emb_v[index // (VOC // BLOCK), pl.ds((index % (VOC // BLOCK)) * BLOCK, BLOCK), :]
        out[...] = lax.dot_general(
            block, states[...], (((1,), (1,)), ((), ())), preferred_element_type=jnp.float32
        )

    def totals(index, out, carry):
        total, picked = carry
        capped = jnp.tanh(out[...] * (1.0 / 30.0)) * 30.0
        total = total + fold(jnp.exp(capped))
        picked = picked + fold(jnp.where(row + index * BLOCK == targets, capped, 0.0))
        return total, picked

    loads[3].wait()
    pair[1].wait_recv()
    zero = jnp.zeros((8, CHIPS * DRAFT), jnp.float32)
    product(0, even)

    def step(k, carry):
        product(2 * k + 1, odd)
        carry = totals(2 * k, even, carry)
        product(2 * k + 2, even)
        return totals(2 * k + 1, odd, carry)

    blocks = 2 * VOC // BLOCK
    carry = lax.fori_loop(0, blocks // 2 - 1, step, (zero, zero))
    product(blocks - 1, odd)
    carry = totals(blocks - 2, even, carry)
    total, picked = totals(blocks - 1, odd, carry)
    total = jnp.sum(total, axis=0, keepdims=True)
    picked = jnp.sum(picked, axis=0, keepdims=True)
    for k in range(4):
        res_out[k, 0:1, :] = total[:, 128 * k : 128 * k + 128]
        res_out[k, 1:2, :] = picked[:, 128 * k : 128 * k + 128]

    def send_results(step, carry):
        to = (chip + step) % CHIPS
        pltpu.make_async_remote_copy(
            src_ref=res_out.at[to // 16],
            dst_ref=res_in.at[chip],
            send_sem=res_sem.at[0],
            recv_sem=res_sem.at[1],
            device_id=(to * 2 + core,),
            device_id_type=MESH,
        ).start()
        return carry

    lax.fori_loop(1, CHIPS, send_results, 0)
    res_in[chip] = res_out[chip // 16]

    for copy in sent:
        copy.wait_send()
    for copy in pair:
        copy.wait_send()

    def wait_sent(ref, sem):
        pltpu.make_async_copy(ref, ref, sem).wait()

    wait_sent(inbox.at[most], id_sem.at[0])
    wait_sent(packed.at[most], row_sem.at[0])
    wait_sent(res_in.at[most], res_sem.at[0])
    wait_all(res_in, res_sem.at[1])
    summed = jnp.sum(res_in[...], axis=0)
    summed = pltpu.roll(summed, (128 - (chip % 16) * DRAFT) % 128, 1)
    score = summed[1:2, :] - jnp.log(summed[0:1, :])
    keep = lane < jnp.minimum(jnp.minimum(acc_s[0], len_s[0]), DRAFT)
    score = jnp.where(keep, score, 0.0)
    tok_ref[...] = score[:, 0:DRAFT]
    seq_ref[0] = jnp.sum(score)


def per_device(
    draft_ids,
    draft_len,
    accepted,
    targets,
    hidden,
    ple_table,
    gate_proj,
    out_proj,
    post_gain,
    final_gain,
    embedding,
):
    smem = pl.BlockSpec(memory_space=pltpu.SMEM)
    vmem = pl.BlockSpec(memory_space=pltpu.VMEM)
    hbm = pl.BlockSpec(memory_space=pl.ANY)
    tokens = CHIPS * DRAFT
    return pl.pallas_call(
        kernel,
        out_shape=(
            jax.ShapeDtypeStruct((1, DRAFT), jnp.float32),
            jax.ShapeDtypeStruct((1,), jnp.float32),
        ),
        in_specs=[smem] * 4 + [vmem] * 3 + [hbm] * 4,
        out_specs=(vmem, smem),
        scratch_shapes=[
            pltpu.VMEM((2, VOC, D), jnp.bfloat16),
            pltpu.VMEM((2, VOC, 2 * PLE), jnp.bfloat16),
            pltpu.VMEM((2, D, PLE), jnp.bfloat16),
            pltpu.VMEM((2, PLE, D), jnp.bfloat16),
            pltpu.VMEM((1, 256), jnp.int32),
            pltpu.VMEM((CHIPS, 1, 256), jnp.int32),
            pltpu.VMEM((CHIPS * 16, 128), jnp.float32),
            pltpu.VMEM((CHIPS, 16, 128), jnp.bfloat16),
            pltpu.VMEM((CHIPS, 16, 128), jnp.bfloat16),
            pltpu.VMEM((4, 4, 4, DRAFT, D), jnp.bfloat16),
            pltpu.VMEM((tokens, D), jnp.bfloat16),
            pltpu.VMEM((BLOCK, tokens), jnp.float32),
            pltpu.VMEM((BLOCK, tokens), jnp.float32),
            pltpu.VMEM((4, 2, 128), jnp.float32),
            pltpu.VMEM((CHIPS, 2, 128), jnp.float32),
            pltpu.SemaphoreType.DMA((4,)),
            pltpu.SemaphoreType.DMA((2,)),
            pltpu.SemaphoreType.DMA((2,)),
            pltpu.SemaphoreType.DMA((2,)),
            pltpu.SemaphoreType.DMA((2,)),
            pltpu.SemaphoreType.DMA((2,)),
            pltpu.SemaphoreType.DMA((33,)),
            pltpu.SemaphoreType.DMA((3, 11)),
        ],
        compiler_params=pltpu.CompilerParams(
            collective_id=0, has_side_effects=True, vmem_limit_bytes=60 * 1024 * 1024
        ),
        name="verify",
    )(
        draft_ids,
        targets,
        draft_len,
        accepted,
        hidden,
        post_gain,
        final_gain,
        ple_table,
        gate_proj,
        out_proj,
        embedding,
    )


def solution(mesh):
    one, two, three = P("vocab"), P("vocab", None), P("vocab", None, None)
    return jax.shard_map(
        per_device,
        mesh=mesh,
        in_specs=(two, one, one, two, three, two, P(), P(), P(), P(), two),
        out_specs=(two, one),
        check_vma=False,
    )
```
